32 devices in a mesh: texel: 8 (over y, x, core), light: 4 (over z).
Axes of the slice: x: 2, y: 2, z: 4, core: 2. Of those that a mesh axis runs over, the one named last changes fastest.
Arguments:
- tex_feat: bfloat16 [8192, 512], P('texel'), may hold values from -18 to 18
- light_feat: bfloat16 [6144, 512], P('light'), may hold values from -0.25 to 0.25
- sketch: bfloat16 [6144, 256], P('light'), may hold values from -0.078125 to 0.078125
- row_counts: int32 [8], replicated, may hold values from 1 to 1024, 4096 in all
Outputs:
- basis: float32 [8192, 256], P('texel')
- coeffs: float32 [256, 6144], P('texel', 'light')
The draws below stay inside these ranges and needn't reach their ends.
Inputs may be any that keep to these rules, and one draw needn't show every extreme that they name: row_counts sums to 8 * 512; some entry equals 1024.
All inputs are finite; a program needn't handle non-finite values.
Results may differ from the reference program's by a relative error of at most 0.0034.
Values sent between devices are 32-bit elements; how exact they have to be, the bound alone decides.
A program may use at most 64 MiB of HBM per device.

```python
import math
import jax
import jax.numpy as jnp
import numpy as np
from jax import lax

F = 512
K = 256
CAP = 1024
LIGHT_DEV = 1536
TEX_SLOTS = 8192
LIGHTS = 6144
N_TEXEL = 8
N_LIGHT = 4


def level_of(key, extent, cuts, low, largest):
    def one(axis_at, parts):
        heights = jax.random.uniform(jax.random.fold_in(jax.random.fold_in(key, 6), axis_at), (parts,), jnp.float32, low / len(cuts), largest / len(cuts))
        return jnp.repeat(jnp.exp(heights), extent[axis_at] // parts).reshape((-1,) + (1,) * (len(extent) - axis_at - 1))

    factor_of = one(*cuts[0])
    for cut in cuts[1:]:
        factor_of = factor_of * one(*cut)
    return factor_of


def split_up(count, total, reach, slope):
    loads = [(1 << 20) // math.isqrt(grade ** slope) + 1 for grade in range(2, count + 1)]
    surplus, counts = total - reach - (count - 1), [1] * (count - 1)
    while surplus > 0:
        free = [i for i in range(count - 1) if counts[i] < reach]
        mass, remaining = sum([loads[i] for i in free]), surplus
        for i in free:
            extra = min(reach - counts[i], max(1, remaining * loads[i] // mass), surplus)
            counts[i] = counts[i] + extra
            surplus = surplus - extra
    return np.array([reach] + counts)


def ragged_sizes(own_key, amount, total, bound, slope):
    if amount == 2:
        one = jax.random.randint(own_key, (), max(1, total - bound), min(bound, total - 1) + 1)
        return jnp.stack([one, total - one])
    tallies = jnp.asarray(split_up(amount, total, bound, slope), jnp.int32)
    twos = (amount - 1) // 2
    source_of, sink = tallies[1:1 + 2 * twos:2], tallies[2:2 + 2 * twos:2]
    margin = jnp.minimum(source_of - 1, bound - sink)
    passed = jax.random.randint(jax.random.fold_in(own_key, 1), (twos,), 0, 1 << 20) % (margin + 1)
    tallies = tallies.at[1:1 + 2 * twos:2].set(source_of - passed).at[2:2 + 2 * twos:2].set(sink + passed)
    return tallies[jax.random.permutation(jax.random.fold_in(own_key, 2), amount)]


def scatter_about(key, dims, scale, limit, split=(), kind=jnp.bfloat16):
    factor_of = level_of(key, dims, split, -0.22, 0.18) if split else 1.0
    entries = jax.random.normal(key, dims, jnp.float32) * scale * factor_of
    return jnp.minimum(jnp.maximum(entries, -limit), limit).astype(kind)


def setup_inputs(seed: int = 0) -> dict:
    arg_keys = jax.random.split(jax.random.key(seed), 5)
    return {
        "tex_feat": scatter_about(arg_keys[0], (TEX_SLOTS, F), 3.0, 18.0, ((0, 8),)),
        "light_feat": scatter_about(arg_keys[1], (LIGHTS, F), F ** -0.5, 0.25, ((0, 4),)),
        "sketch": scatter_about(arg_keys[2], (LIGHTS, K), LIGHTS ** -0.5, 0.078125, ((0, 4),)),
        "row_counts": ragged_sizes(arg_keys[3], N_TEXEL, N_TEXEL * CAP // 2, CAP, 2).astype(jnp.int32),
    }


def reference(tex_feat, light_feat, sketch, row_counts):
    slot_total = tex_feat.shape[0]
    positions = lax.iota(jnp.int32, slot_total)
    owners = (positions // CAP).astype(jnp.int32)
    row_valid = (positions % CAP < row_counts[owners]).astype(jnp.float32)
    valid_total = jnp.sum(row_counts).astype(jnp.float32)
    light_blocks = light_feat.reshape(N_LIGHT, LIGHT_DEV, F)
    sketch_blocks = sketch.reshape(N_LIGHT, LIGHT_DEV, K)

    def make_tiles(feats):
        logits = lax.dot_general(tex_feat.astype(jnp.float32), feats.astype(jnp.float32), (((1,), (1,)), ((), ())), preferred_element_type=jnp.float32)
        return jnp.sin(logits).astype(jnp.bfloat16)

    def accumulate(carry, pair):
        feats, block = pair
        return (carry + jnp.dot(make_tiles(feats).astype(jnp.float32), block.astype(jnp.float32), preferred_element_type=jnp.float32), None)
    sketched, _ = lax.scan(accumulate, jnp.zeros((slot_total, K), jnp.float32), (light_blocks, sketch_blocks))
    sketched = sketched * row_valid[:, None]
    gram_matrix = jnp.dot(sketched.T, sketched, precision=lax.Precision.HIGHEST) / valid_total
    factor = jnp.linalg.cholesky(gram_matrix)
    basis = jax.scipy.linalg.solve_triangular(factor, sketched.T, lower=True).T
    basis_half = basis.astype(jnp.bfloat16)

    def project(feats):
        return lax.dot_general(basis_half.astype(jnp.float32), make_tiles(feats).astype(jnp.float32), (((0,), (0,)), ((), ())), preferred_element_type=jnp.float32)
    coeff_blocks = lax.map(project, light_blocks)
    coeffs = jnp.transpose(coeff_blocks, (1, 0, 2)).reshape(K, N_LIGHT * LIGHT_DEV) / jnp.sqrt(valid_total)
    return (basis, coeffs)
```

```python
import functools

import jax
import jax.numpy as jnp
from jax import lax
from jax.experimental import pallas as pl
from jax.experimental.pallas import tpu as pltpu
from jax.sharding import PartitionSpec as P

HIGHEST = lax.Precision.HIGHEST
BLOCK = 64
INV_TWO_PI = 0.15915494309189535
TWO_PI_HIGH = 6.28125
TWO_PI_LOW = 0.001935307179586232
SINE = (
    0.9999999944783076,
    -0.16666664569596037,
    0.008333310280569169,
    -0.00019840151040396647,
    2.752937413742719e-06,
    -2.4676261406891767e-08,
    1.344908473337278e-10,
)


def bounded_sine(x):
    turns = jnp.round(x * INV_TWO_PI)
    r = (x - turns * TWO_PI_HIGH) - turns * TWO_PI_LOW
    s = r * r
    value = jnp.full_like(s, SINE[-1])
    for coefficient in SINE[-2::-1]:
        value = value * s + coefficient
    return value * r


def eliminate(block):
    rows = [block[8 * t : 8 * t + 8, :] for t in range(8)]
    below = lax.broadcasted_iota(jnp.int32, (8, 128), 0)
    for p in range(8):
        columns = {
            (t, k): jnp.broadcast_to(rows[t][:, 8 * p + k : 8 * p + k + 1], (8, 128))
            for t in range(p, 8)
            for k in range(8)
        }
        for k in range(8):
            inverse = 1.0 / jnp.broadcast_to(columns[p, k][k : k + 1, :], (8, 128))
            pivot_row = jnp.broadcast_to(rows[p][k : k + 1, :], (8, 128))
            entries = [
                jnp.broadcast_to(columns[p, later][k : k + 1, :], (8, 128))
                for later in range(k + 1, 8)
            ]
            for t in range(p, 8):
                factor = columns[t, k] * inverse
                if t == p:
                    factor = jnp.where(below > k, factor, 0.0)
                rows[t] = rows[t] - factor * pivot_row
                for later in range(k + 1, 8):
                    columns[t, later] = columns[t, later] - factor * entries[later - k - 1]
    return jnp.concatenate(rows, axis=0)


def factor_inverse(gram_ref, inverse_ref, work_ref):
    size = gram_ref.shape[0]
    work_ref[...] = gram_ref[...]
    row = lax.broadcasted_iota(jnp.int32, (size, size), 0)
    column = lax.broadcasted_iota(jnp.int32, (size, size), 1)
    inverse_ref[...] = jnp.where(row == column, 1.0, 0.0).astype(jnp.float32)
    lane = lax.broadcasted_iota(jnp.int32, (BLOCK, 128), 1)
    line = lax.broadcasted_iota(jnp.int32, (BLOCK, 128), 0)
    for start in range(0, size, BLOCK):
        own = slice(start, start + BLOCK)
        tile_start = start // 128 * 128
        tile = work_ref[own, tile_start : tile_start + 128]
        if start % 128:
            tile = pltpu.roll(tile, 64, 1)
        unit = jnp.where(lane - BLOCK == line, 1.0, 0.0)
        done = eliminate(jnp.where(lane < BLOCK, tile, unit))
        pivots = jnp.sum(jnp.where(lane == line, done, 0.0), axis=1, keepdims=True)
        scaled = pltpu.roll(done * lax.rsqrt(pivots), 64, 1)[:, :BLOCK]
        left = jnp.dot(scaled, work_ref[own, :], precision=HIGHEST, preferred_element_type=jnp.float32)
        right = jnp.dot(scaled, inverse_ref[own, :], precision=HIGHEST, preferred_element_type=jnp.float32)
        inverse_ref[own, :] = right
        rest = size - start - BLOCK
        if rest:
            lower = slice(start + BLOCK, size)
            flipped = left.T[start + BLOCK :, :]
            work_ref[lower, :] -= jnp.dot(flipped, left, precision=HIGHEST, preferred_element_type=jnp.float32)
            inverse_ref[lower, :] -= jnp.dot(flipped, right, precision=HIGHEST, preferred_element_type=jnp.float32)


def inverse_of_factor(gram):
    size = gram.shape[0]
    return pl.pallas_call(
        factor_inverse,
        out_shape=jax.ShapeDtypeStruct((size, size), jnp.float32),
        in_specs=[pl.BlockSpec(memory_space=pltpu.VMEM)],
        out_specs=pl.BlockSpec(memory_space=pltpu.VMEM),
        scratch_shapes=[pltpu.VMEM((size, size), jnp.float32)],
    )(gram)


def on_device(tex_feat, light_feat, sketch, row_counts):
    capacity = tex_feat.shape[0]
    own_count = row_counts[lax.axis_index("texel")]
    valid_total = jnp.sum(row_counts).astype(jnp.float32)
    logits = lax.dot_general(
        tex_feat, light_feat, (((1,), (1,)), ((), ())), preferred_element_type=jnp.float32
    )
    tile_block = bounded_sine(logits).astype(jnp.bfloat16)
    row_valid = (lax.iota(jnp.int32, capacity) < own_count).astype(jnp.float32)
    partial_value = (
        jnp.dot(tile_block, sketch, preferred_element_type=jnp.float32) * row_valid[:, None]
    )
    sketched = lax.psum(partial_value, "light")
    gram_local = jnp.dot(sketched.T, sketched, precision=HIGHEST)
    gram_matrix = lax.psum(gram_local, "texel") / valid_total
    inverse = inverse_of_factor(gram_matrix)
    basis = lax.dot_general(sketched, inverse, (((1,), (1,)), ((), ())), precision=HIGHEST)
    basis_half = basis.astype(jnp.bfloat16)
    coeffs = lax.psum_scatter(
        lax.dot_general(
            basis_half, tile_block, (((0,), (0,)), ((), ())), preferred_element_type=jnp.float32
        ),
        "texel",
        scatter_dimension=0,
        tiled=True,
    ) / jnp.sqrt(valid_total)
    return (basis, coeffs)


def solution(mesh):
    placed = (P("texel", None), P("light", None), P("light", None), P())
    return jax.shard_map(
        on_device,
        mesh=mesh,
        in_specs=placed,
        out_specs=(P("texel", None), P("texel", "light")),
        check_vma=False,
    )
```

```python
import functools

import jax
import jax.numpy as jnp
from jax import lax
from jax.experimental import pallas as pl
from jax.experimental.pallas import tpu as pltpu
from jax.sharding import PartitionSpec as P

HIGHEST = lax.Precision.HIGHEST
BLOCK = 64
INV_TWO_PI = 0.15915494309189535
TWO_PI_HIGH = 6.28125
TWO_PI_LOW = 0.001935307179586232
SINE = (
    0.9999999944783076,
    -0.16666664569596037,
    0.008333310280569169,
    -0.00019840151040396647,
    2.752937413742719e-06,
    -2.4676261406891767e-08,
    1.344908473337278e-10,
)


def bounded_sine(x):
    turns = jnp.round(x * INV_TWO_PI)
    r = (x - turns * TWO_PI_HIGH) - turns * TWO_PI_LOW
    s = r * r
    value = jnp.full_like(s, SINE[-1])
    for coefficient in SINE[-2::-1]:
        value = value * s + coefficient
    return value * r


def eliminate(block):
    rows = [block[8 * t : 8 * t + 8, :] for t in range(8)]
    below = lax.broadcasted_iota(jnp.int32, (8, 128), 0)
    for p in range(8):
        columns = {
            (t, k): jnp.broadcast_to(rows[t][:, 8 * p + k : 8 * p + k + 1], (8, 128))
            for t in range(p, 8)
            for k in range(8)
        }
        for k in range(8):
            inverse = 1.0 / jnp.broadcast_to(columns[p, k][k : k + 1, :], (8, 128))
            pivot_row = jnp.broadcast_to(rows[p][k : k + 1, :], (8, 128))
            entries = [
                jnp.broadcast_to(columns[p, later][k : k + 1, :], (8, 128))
                for later in range(k + 1, 8)
            ]
            for t in range(p, 8):
                factor = columns[t, k] * inverse
                if t == p:
                    factor = jnp.where(below > k, factor, 0.0)
                rows[t] = rows[t] - factor * pivot_row
                for later in range(k + 1, 8):
                    columns[t, later] = columns[t, later] - factor * entries[later - k - 1]
    return jnp.concatenate(rows, axis=0)


def factor_inverse(gram_ref, inverse_ref, work_ref):
    size = gram_ref.shape[0]
    work_ref[...] = gram_ref[...]
    row = lax.broadcasted_iota(jnp.int32, (size, size), 0)
    column = lax.broadcasted_iota(jnp.int32, (size, size), 1)
    inverse_ref[...] = jnp.where(row == column, 1.0, 0.0).astype(jnp.float32)
    lane = lax.broadcasted_iota(jnp.int32, (BLOCK, 128), 1)
    line = lax.broadcasted_iota(jnp.int32, (BLOCK, 128), 0)
    for start in range(0, size, BLOCK):
        own = slice(start, start + BLOCK)
        tile_start = start // 128 * 128
        tile = work_ref[own, tile_start : tile_start + 128]
        if start % 128:
            tile = pltpu.roll(tile, 64, 1)
        unit = jnp.where(lane - BLOCK == line, 1.0, 0.0)
        done = eliminate(jnp.where(lane < BLOCK, tile, unit))
        pivots = jnp.sum(jnp.where(lane == line, done, 0.0), axis=1, keepdims=True)
        scaled = pltpu.roll(done * lax.rsqrt(pivots), 64, 1)[:, :BLOCK]
        left = jnp.dot(scaled, work_ref[own, :], precision=HIGHEST, preferred_element_type=jnp.float32)
        right = jnp.dot(scaled, inverse_ref[own, :], precision=HIGHEST, preferred_element_type=jnp.float32)
        inverse_ref[own, :] = right
        rest = size - start - BLOCK
        if rest:
            lower = slice(start + BLOCK, size)
            flipped = left.T[start + BLOCK :, :]
            work_ref[lower, :] -= jnp.dot(flipped, left, precision=HIGHEST, preferred_element_type=jnp.float32)
            inverse_ref[lower, :] -= jnp.dot(flipped, right, precision=HIGHEST, preferred_element_type=jnp.float32)


def inverse_of_factor(gram):
    size = gram.shape[0]
    return pl.pallas_call(
        factor_inverse,
        out_shape=jax.ShapeDtypeStruct((size, size), jnp.float32),
        in_specs=[pl.BlockSpec(memory_space=pltpu.VMEM)],
        out_specs=pl.BlockSpec(memory_space=pltpu.VMEM),
        scratch_shapes=[pltpu.VMEM((size, size), jnp.float32)],
    )(gram)


MESH_ID = pl.DeviceIdType.MESH


def greet(peers):
    barrier = pltpu.get_barrier_semaphore()
    for peer in peers:
        pl.semaphore_signal(barrier, inc=1, device_id=peer, device_id_type=MESH_ID)
    pl.semaphore_wait(barrier, len(peers))


def sketch_and_gram(
    n_texel, n_light, partial_ref, whole_ref, gram_ref,
    landed, whole, pieces, plane, column, gram,
    part_send, part_recv, plane_send, plane_recv, column_send, column_recv,
    full_send, full_recv, row_send, row_recv,
):
    texel, light = lax.axis_index("texel"), lax.axis_index("light")
    depth = partial_ref.shape[0] // n_light
    size = partial_ref.shape[1]
    piece = size // n_texel
    lights = [lax.rem(light + d, n_light) for d in range(n_light)]
    texels = [lax.rem(texel + d, n_texel) for d in range(n_texel)]
    greet([(texel, lights[d]) for d in range(1, n_light)] + [(texels[d], light) for d in range(1, n_texel)])

    def send(source, target, send_sem, recv_sem, device):
        copy = pltpu.make_async_remote_copy(
            src_ref=source, dst_ref=target, send_sem=send_sem, recv_sem=recv_sem,
            device_id=device, device_id_type=MESH_ID,
        )
        copy.start()
        return copy

    def rows_of(index, height):
        return pl.ds(pl.multiple_of(index * height, height), height)

    copies = [
        send(
            partial_ref.at[rows_of(lights[d], depth)], landed.at[d],
            part_send.at[d], part_recv.at[d], (texel, lights[d]),
        )
        for d in range(1, n_light)
    ]
    own = partial_ref[rows_of(light, depth), :]
    for d, copy in enumerate(copies, 1):
        copy.wait()
        own = own + landed[d]
    whole[rows_of(light, depth), :] = own

    local = lax.dot_general(
        own, own, (((0,), (0,)), ((), ())), precision=HIGHEST, preferred_element_type=jnp.float32
    )
    for index in range(n_texel):
        pieces[index] = local[index * piece : (index + 1) * piece, :]
    copies = [
        send(pieces.at[texels[d]], plane.at[d], plane_send.at[d], plane_recv.at[d], (texels[d], light))
        for d in range(1, n_texel)
    ]
    total = pieces[texel]
    for d, copy in enumerate(copies, 1):
        copy.wait()
        total = total + plane[d]
    column[light] = total
    copies = [
        send(column.at[light], column.at[light], column_send.at[d], column_recv.at[d], (texel, lights[d]))
        for d in range(1, n_light)
    ]
    for copy in copies:
        copy.wait()
    gathers = [
        send(
            whole.at[rows_of(light, depth)], whole.at[rows_of(light, depth)],
            full_send.at[d], full_recv.at[d], (texel, lights[d]),
        )
        for d in range(1, n_light)
    ]
    total = column[0]
    for index in range(1, n_light):
        total = total + column[index]
    gram[rows_of(texel, piece), :] = total
    copies = [
        send(
            gram.at[rows_of(texel, piece)], gram.at[rows_of(texel, piece)],
            row_send.at[d], row_recv.at[d], (texels[d], light),
        )
        for d in range(1, n_texel)
    ]
    for copy in copies:
        copy.wait()
    gram_ref[...] = gram[...]
    for copy in gathers:
        copy.wait()
    whole_ref[...] = whole[...]


def reduced(partial, n_texel, n_light):
    capacity, size = partial.shape
    depth, piece = capacity // n_light, size // n_texel
    vmem = pl.BlockSpec(memory_space=pltpu.VMEM)
    f32 = jnp.float32
    sems = pltpu.SemaphoreType.DMA
    return pl.pallas_call(
        functools.partial(sketch_and_gram, n_texel, n_light),
        out_shape=(
            jax.ShapeDtypeStruct((capacity, size), f32),
            jax.ShapeDtypeStruct((size, size), f32),
        ),
        in_specs=[vmem],
        out_specs=(vmem, vmem),
        scratch_shapes=[
            pltpu.VMEM((n_light, depth, size), f32),
            pltpu.VMEM((capacity, size), f32),
            pltpu.VMEM((n_texel, piece, size), f32),
            pltpu.VMEM((n_texel, piece, size), f32),
            pltpu.VMEM((n_light, piece, size), f32),
            pltpu.VMEM((size, size), f32),
            sems((n_light,)), sems((n_light,)),
            sems((n_texel,)), sems((n_texel,)),
            sems((n_light,)), sems((n_light,)),
            sems((n_light,)), sems((n_light,)),
            sems((n_texel,)), sems((n_texel,)),
        ],
        compiler_params=pltpu.CompilerParams(collective_id=1, has_side_effects=True),
    )(partial)


def halving_order(bits, last_first):
    rest = list(range(1, bits))
    return [0] + (rest[::-1] if last_first else rest)


def scatter_sum(n_texel, partial_ref, out_ref, held, landed, send_sem, recv_sem):
    texel, light = lax.axis_index("texel"), lax.axis_index("light")
    bits = n_texel.bit_length() - 1
    bit = [lax.rem(texel // (1 << b), 2) for b in range(bits)]
    partner = [texel + (1 - 2 * bit[b]) * (1 << b) for b in range(bits)]
    greet([(partner[b], light) for b in range(bits)])
    piece = partial_ref.shape[0] // n_texel
    width = partial_ref.shape[1] // 2

    def start_of(mask):
        block = 0
        for b in range(bits):
            flipped = 1 - bit[b] if mask >> b & 1 else bit[b]
            block = block + flipped * (1 << b)
        return pl.multiple_of(block * piece, piece)

    orders = [halving_order(bits, False), halving_order(bits, True)]
    flights = [{}, {}]
    for step in range(bits):
        for half, order in enumerate(orders):
            b = order[step]
            left = [m for m in range(n_texel) if all(not m >> done & 1 for done in order[:step])]
            later = order[step + 1 :]
            going = [m for m in left if m >> b & 1]
            going.sort(key=lambda m: [-(m >> c & 1) for c in later])
            columns = pl.ds(half * width, width)
            for m in going:
                kept = m - (1 << b)
                if step == 0:
                    source = partial_ref.at[pl.ds(start_of(m), piece), columns]
                else:
                    arrived = flights[half].pop((step - 1, m))
                    arrived.wait()
                    below = (
                        partial_ref[pl.ds(start_of(m), piece), columns] if step == 1 else held[half, m]
                    )
                    held[half, m] = below + landed[half, step - 1, m]
                    source = held.at[half, m]
                copy = pltpu.make_async_remote_copy(
                    src_ref=source,
                    dst_ref=landed.at[half, step, kept],
                    send_sem=send_sem.at[half, step, kept],
                    recv_sem=recv_sem.at[half, step, kept],
                    device_id=(partner[b], light),
                    device_id_type=MESH_ID,
                )
                copy.start()
                flights[half][step, kept] = copy
        if step:
            for half, order in enumerate(orders):
                for key in [k for k in flights[half] if k[0] == step - 1]:
                    m = key[1]
                    flights[half].pop(key).wait()
                    columns = pl.ds(half * width, width)
                    below = (
                        partial_ref[pl.ds(start_of(m), piece), columns] if step == 1 else held[half, m]
                    )
                    held[half, m] = below + landed[half, step - 1, m]
    for half in range(2):
        columns = pl.ds(half * width, width)
        flights[half].pop((bits - 1, 0)).wait()
        below = partial_ref[pl.ds(start_of(0), piece), columns] if bits == 1 else held[half, 0]
        out_ref[:, half * width : (half + 1) * width] = below + landed[half, bits - 1, 0]


def scattered(partial, n_texel):
    size, lights = partial.shape
    piece, width, bits = size // n_texel, lights // 2, n_texel.bit_length() - 1
    vmem = pl.BlockSpec(memory_space=pltpu.VMEM)
    return pl.pallas_call(
        functools.partial(scatter_sum, n_texel),
        out_shape=jax.ShapeDtypeStruct((piece, lights), jnp.float32),
        in_specs=[vmem],
        out_specs=vmem,
        scratch_shapes=[
            pltpu.VMEM((2, n_texel, piece, width), jnp.float32),
            pltpu.VMEM((2, bits, n_texel, piece, width), jnp.float32),
            pltpu.SemaphoreType.DMA((2, bits, n_texel)),
            pltpu.SemaphoreType.DMA((2, bits, n_texel)),
        ],
        compiler_params=pltpu.CompilerParams(collective_id=2, has_side_effects=True),
    )(partial)


def on_device(n_texel, n_light, tex_feat, light_feat, sketch, row_counts):
    capacity = tex_feat.shape[0]
    own_count = row_counts[lax.axis_index("texel")]
    valid_total = jnp.sum(row_counts).astype(jnp.float32)
    logits = lax.dot_general(
        tex_feat, light_feat, (((1,), (1,)), ((), ())), preferred_element_type=jnp.float32
    )
    tile_block = bounded_sine(logits).astype(jnp.bfloat16)
    row_valid = (lax.iota(jnp.int32, capacity) < own_count).astype(jnp.float32)
    partial_value = (
        jnp.dot(tile_block, sketch, preferred_element_type=jnp.float32) * row_valid[:, None]
    )
    sketched, gram_sum = reduced(partial_value, n_texel, n_light)
    gram_matrix = gram_sum / valid_total
    inverse = inverse_of_factor(gram_matrix)
    basis = lax.dot_general(sketched, inverse, (((1,), (1,)), ((), ())), precision=HIGHEST)
    basis_half = basis.astype(jnp.bfloat16)
    partial_coeffs = lax.dot_general(
        basis_half, tile_block, (((0,), (0,)), ((), ())), preferred_element_type=jnp.float32
    )
    coeffs = scattered(partial_coeffs, n_texel) / jnp.sqrt(valid_total)
    return (basis, coeffs)


def solution(mesh):
    placed = (P("texel", None), P("light", None), P("light", None), P())
    return jax.shard_map(
        functools.partial(on_device, mesh.shape["texel"], mesh.shape["light"]),
        mesh=mesh,
        in_specs=placed,
        out_specs=(P("texel", None), P("texel", "light")),
        check_vma=False,
    )
```

```python
import functools

import jax
import jax.numpy as jnp
from jax import lax
from jax.experimental import pallas as pl
from jax.experimental.pallas import tpu as pltpu
from jax.sharding import PartitionSpec as P

HIGHEST = lax.Precision.HIGHEST
BLOCK = 64
INV_TWO_PI = 0.15915494309189535
TWO_PI_HIGH = 6.28125
TWO_PI_LOW = 0.001935307179586232
SINE = (
    0.9999999944783076,
    -0.16666664569596037,
    0.008333310280569169,
    -0.00019840151040396647,
    2.752937413742719e-06,
    -2.4676261406891767e-08,
    1.344908473337278e-10,
)


def bounded_sine(x):
    turns = jnp.round(x * INV_TWO_PI)
    r = (x - turns * TWO_PI_HIGH) - turns * TWO_PI_LOW
    s = r * r
    value = jnp.full_like(s, SINE[-1])
    for coefficient in SINE[-2::-1]:
        value = value * s + coefficient
    return value * r


def eliminate(block):
    rows = [block[8 * t : 8 * t + 8, :] for t in range(8)]
    below = lax.broadcasted_iota(jnp.int32, (8, 128), 0)
    for p in range(8):
        columns = {
            (t, k): jnp.broadcast_to(rows[t][:, 8 * p + k : 8 * p + k + 1], (8, 128))
            for t in range(p, 8)
            for k in range(8)
        }
        for k in range(8):
            inverse = 1.0 / jnp.broadcast_to(columns[p, k][k : k + 1, :], (8, 128))
            pivot_row = jnp.broadcast_to(rows[p][k : k + 1, :], (8, 128))
            entries = [
                jnp.broadcast_to(columns[p, later][k : k + 1, :], (8, 128))
                for later in range(k + 1, 8)
            ]
            for t in range(p, 8):
                factor = columns[t, k] * inverse
                if t == p:
                    factor = jnp.where(below > k, factor, 0.0)
                rows[t] = rows[t] - factor * pivot_row
                for later in range(k + 1, 8):
                    columns[t, later] = columns[t, later] - factor * entries[later - k - 1]
    return jnp.concatenate(rows, axis=0)


def factor_inverse(gram_ref, inverse_ref, work_ref):
    size = gram_ref.shape[0]
    work_ref[...] = gram_ref[...]
    row = lax.broadcasted_iota(jnp.int32, (size, size), 0)
    column = lax.broadcasted_iota(jnp.int32, (size, size), 1)
    inverse_ref[...] = jnp.where(row == column, 1.0, 0.0).astype(jnp.float32)
    lane = lax.broadcasted_iota(jnp.int32, (BLOCK, 128), 1)
    line = lax.broadcasted_iota(jnp.int32, (BLOCK, 128), 0)
    for start in range(0, size, BLOCK):
        own = slice(start, start + BLOCK)
        tile_start = start // 128 * 128
        tile = work_ref[own, tile_start : tile_start + 128]
        if start % 128:
            tile = pltpu.roll(tile, 64, 1)
        unit = jnp.where(lane - BLOCK == line, 1.0, 0.0)
        done = eliminate(jnp.where(lane < BLOCK, tile, unit))
        pivots = jnp.sum(jnp.where(lane == line, done, 0.0), axis=1, keepdims=True)
        scaled = pltpu.roll(done * lax.rsqrt(pivots), 64, 1)[:, :BLOCK]
        left = jnp.dot(scaled, work_ref[own, :], precision=HIGHEST, preferred_element_type=jnp.float32)
        right = jnp.dot(scaled, inverse_ref[own, :], precision=HIGHEST, preferred_element_type=jnp.float32)
        inverse_ref[own, :] = right
        rest = size - start - BLOCK
        if rest:
            lower = slice(start + BLOCK, size)
            flipped = left.T[start + BLOCK :, :]
            work_ref[lower, :] -= jnp.dot(flipped, left, precision=HIGHEST, preferred_element_type=jnp.float32)
            inverse_ref[lower, :] -= jnp.dot(flipped, right, precision=HIGHEST, preferred_element_type=jnp.float32)


MESH_ID = pl.DeviceIdType.MESH


def greet(peers):
    barrier = pltpu.get_barrier_semaphore()
    for peer in peers:
        pl.semaphore_signal(barrier, inc=1, device_id=peer, device_id_type=MESH_ID)
    pl.semaphore_wait(barrier, len(peers))


def sketch_and_gram(
    n_texel, n_light, partial_ref, count_ref, whole_ref, inverse_ref,
    landed, whole, pieces, plane, column, gram, scaled, work,
    part_send, part_recv, plane_send, plane_recv, column_send, column_recv,
    full_send, full_recv, row_send, row_recv,
):
    texel, light = lax.axis_index("texel"), lax.axis_index("light")
    depth = partial_ref.shape[0] // n_light
    size = partial_ref.shape[1]
    piece = size // n_texel
    lights = [lax.rem(light + d, n_light) for d in range(n_light)]
    texels = [lax.rem(texel + d, n_texel) for d in range(n_texel)]
    greet([(texel, lights[d]) for d in range(1, n_light)] + [(texels[d], light) for d in range(1, n_texel)])

    def send(source, target, send_sem, recv_sem, device):
        copy = pltpu.make_async_remote_copy(
            src_ref=source, dst_ref=target, send_sem=send_sem, recv_sem=recv_sem,
            device_id=device, device_id_type=MESH_ID,
        )
        copy.start()
        return copy

    def rows_of(index, height):
        return pl.ds(pl.multiple_of(index * height, height), height)

    copies = [
        send(
            partial_ref.at[rows_of(lights[d], depth)], landed.at[d],
            part_send.at[d], part_recv.at[d], (texel, lights[d]),
        )
        for d in range(1, n_light)
    ]
    own = partial_ref[rows_of(light, depth), :]
    for d, copy in enumerate(copies, 1):
        copy.wait()
        own = own + landed[d]
    whole[rows_of(light, depth), :] = own
    early = depth // 4

    def gather(part, first, height):
        rows = pl.ds(pl.multiple_of(light * depth + first, 8), height)
        return [
            send(
                whole.at[rows], whole.at[rows], full_send.at[part, d], full_recv.at[part, d], (texel, lights[d])
            )
            for d in range(1, n_light)
        ]

    gathers = gather(0, 0, early)
    local = lax.dot_general(
        own, own, (((0,), (0,)), ((), ())), precision=HIGHEST, preferred_element_type=jnp.float32
    )
    for index in range(n_texel):
        pieces[index] = local[index * piece : (index + 1) * piece, :]
    copies = [
        send(pieces.at[texels[d]], plane.at[d], plane_send.at[d], plane_recv.at[d], (texels[d], light))
        for d in range(1, n_texel)
    ]
    total = pieces[texel]
    for d, copy in enumerate(copies, 1):
        copy.wait()
        total = total + plane[d]
    column[light] = total
    copies = [
        send(column.at[light], column.at[light], column_send.at[d], column_recv.at[d], (texel, lights[d]))
        for d in range(1, n_light)
    ]
    for copy in copies:
        copy.wait()
    gathers += gather(1, early, depth - early)
    total = column[0]
    for index in range(1, n_light):
        total = total + column[index]
    gram[rows_of(texel, piece), :] = total
    copies = [
        send(
            gram.at[rows_of(texel, piece)], gram.at[rows_of(texel, piece)],
            row_send.at[d], row_recv.at[d], (texels[d], light),
        )
        for d in range(1, n_texel)
    ]
    for copy in copies:
        copy.wait()
    scaled[...] = gram[...] / count_ref[...]
    factor_inverse(scaled, inverse_ref, work)
    for copy in gathers:
        copy.wait()
    whole_ref[...] = whole[...]


def reduced(partial, count, n_texel, n_light):
    capacity, size = partial.shape
    depth, piece = capacity // n_light, size // n_texel
    vmem = pl.BlockSpec(memory_space=pltpu.VMEM)
    f32 = jnp.float32
    sems = pltpu.SemaphoreType.DMA
    return pl.pallas_call(
        functools.partial(sketch_and_gram, n_texel, n_light),
        out_shape=(
            jax.ShapeDtypeStruct((capacity, size), f32),
            jax.ShapeDtypeStruct((size, size), f32),
        ),
        in_specs=[vmem, vmem],
        out_specs=(vmem, vmem),
        scratch_shapes=[
            pltpu.VMEM((n_light, depth, size), f32),
            pltpu.VMEM((capacity, size), f32),
            pltpu.VMEM((n_texel, piece, size), f32),
            pltpu.VMEM((n_texel, piece, size), f32),
            pltpu.VMEM((n_light, piece, size), f32),
            pltpu.VMEM((size, size), f32),
            pltpu.VMEM((size, size), f32),
            pltpu.VMEM((size, size), f32),
            sems((n_light,)), sems((n_light,)),
            sems((n_texel,)), sems((n_texel,)),
            sems((n_light,)), sems((n_light,)),
            sems((2, n_light)), sems((2, n_light)),
            sems((n_texel,)), sems((n_texel,)),
        ],
        compiler_params=pltpu.CompilerParams(collective_id=1, has_side_effects=True),
    )(partial, count)


def halving_order(bits, last_first):
    rest = list(range(1, bits))
    return [0] + (rest[::-1] if last_first else rest)


def scatter_sum(n_texel, partial_ref, out_ref, held, landed, send_sem, recv_sem):
    texel, light = lax.axis_index("texel"), lax.axis_index("light")
    bits = n_texel.bit_length() - 1
    bit = [lax.rem(texel // (1 << b), 2) for b in range(bits)]
    partner = [texel + (1 - 2 * bit[b]) * (1 << b) for b in range(bits)]
    greet([(partner[b], light) for b in range(bits)])
    piece = partial_ref.shape[0] // n_texel
    width = partial_ref.shape[1] // 2

    def start_of(mask):
        block = 0
        for b in range(bits):
            flipped = 1 - bit[b] if mask >> b & 1 else bit[b]
            block = block + flipped * (1 << b)
        return pl.multiple_of(block * piece, piece)

    orders = [halving_order(bits, False), halving_order(bits, True)]
    flights = [{}, {}]
    for step in range(bits):
        for half, order in enumerate(orders):
            b = order[step]
            left = [m for m in range(n_texel) if all(not m >> done & 1 for done in order[:step])]
            later = order[step + 1 :]
            going = [m for m in left if m >> b & 1]
            going.sort(key=lambda m: [-(m >> c & 1) for c in later])
            columns = pl.ds(half * width, width)
            for m in going:
                kept = m - (1 << b)
                if step == 0:
                    source = partial_ref.at[pl.ds(start_of(m), piece), columns]
                else:
                    arrived = flights[half].pop((step - 1, m))
                    arrived.wait()
                    below = (
                        partial_ref[pl.ds(start_of(m), piece), columns] if step == 1 else held[half, m]
                    )
                    held[half, m] = below + landed[half, step - 1, m]
                    source = held.at[half, m]
                copy = pltpu.make_async_remote_copy(
                    src_ref=source,
                    dst_ref=landed.at[half, step, kept],
                    send_sem=send_sem.at[half, step, kept],
                    recv_sem=recv_sem.at[half, step, kept],
                    device_id=(partner[b], light),
                    device_id_type=MESH_ID,
                )
                copy.start()
                flights[half][step, kept] = copy
        if step:
            for half, order in enumerate(orders):
                for key in [k for k in flights[half] if k[0] == step - 1]:
                    m = key[1]
                    flights[half].pop(key).wait()
                    columns = pl.ds(half * width, width)
                    below = (
                        partial_ref[pl.ds(start_of(m), piece), columns] if step == 1 else held[half, m]
                    )
                    held[half, m] = below + landed[half, step - 1, m]
    for half in range(2):
        columns = pl.ds(half * width, width)
        flights[half].pop((bits - 1, 0)).wait()
        below = partial_ref[pl.ds(start_of(0), piece), columns] if bits == 1 else held[half, 0]
        out_ref[:, half * width : (half + 1) * width] = below + landed[half, bits - 1, 0]


def scattered(partial, n_texel):
    size, lights = partial.shape
    piece, width, bits = size // n_texel, lights // 2, n_texel.bit_length() - 1
    vmem = pl.BlockSpec(memory_space=pltpu.VMEM)
    return pl.pallas_call(
        functools.partial(scatter_sum, n_texel),
        out_shape=jax.ShapeDtypeStruct((piece, lights), jnp.float32),
        in_specs=[vmem],
        out_specs=vmem,
        scratch_shapes=[
            pltpu.VMEM((2, n_texel, piece, width), jnp.float32),
            pltpu.VMEM((2, bits, n_texel, piece, width), jnp.float32),
            pltpu.SemaphoreType.DMA((2, bits, n_texel)),
            pltpu.SemaphoreType.DMA((2, bits, n_texel)),
        ],
        compiler_params=pltpu.CompilerParams(collective_id=2, has_side_effects=True),
    )(partial)


def on_device(n_texel, n_light, tex_feat, light_feat, sketch, row_counts):
    capacity = tex_feat.shape[0]
    own_count = row_counts[lax.axis_index("texel")]
    valid_total = jnp.sum(row_counts).astype(jnp.float32)
    logits = lax.dot_general(
        tex_feat, light_feat, (((1,), (1,)), ((), ())), preferred_element_type=jnp.float32
    )
    tile_block = bounded_sine(logits).astype(jnp.bfloat16)
    row_valid = (lax.iota(jnp.int32, capacity) < own_count).astype(jnp.float32)
    partial_value = (
        jnp.dot(tile_block, sketch, preferred_element_type=jnp.float32) * row_valid[:, None]
    )
    count = jnp.full((1, partial_value.shape[1]), valid_total)
    sketched, inverse = reduced(partial_value, count, n_texel, n_light)
    basis = lax.dot_general(sketched, inverse, (((1,), (1,)), ((), ())), precision=HIGHEST)
    basis_half = basis.astype(jnp.bfloat16)
    partial_coeffs = lax.dot_general(
        basis_half, tile_block, (((0,), (0,)), ((), ())), preferred_element_type=jnp.float32
    )
    coeffs = scattered(partial_coeffs, n_texel) / jnp.sqrt(valid_total)
    return (basis, coeffs)


def solution(mesh):
    placed = (P("texel", None), P("light", None), P("light", None), P())
    return jax.shard_map(
        functools.partial(on_device, mesh.shape["texel"], mesh.shape["light"]),
        mesh=mesh,
        in_specs=placed,
        out_specs=(P("texel", None), P("texel", "light")),
        check_vma=False,
    )
```

```python
import functools

import jax
import jax.numpy as jnp
from jax import lax
from jax.experimental import pallas as pl
from jax.experimental.pallas import tpu as pltpu
from jax.sharding import PartitionSpec as P

HIGHEST = lax.Precision.HIGHEST
BLOCK = 64
INV_TWO_PI = 0.15915494309189535
TWO_PI_HIGH = 6.28125
TWO_PI_LOW = 0.001935307179586232
SINE = (
    0.9999999944783076,
    -0.16666664569596037,
    0.008333310280569169,
    -0.00019840151040396647,
    2.752937413742719e-06,
    -2.4676261406891767e-08,
    1.344908473337278e-10,
)


def bounded_sine(x):
    turns = jnp.round(x * INV_TWO_PI)
    r = (x - turns * TWO_PI_HIGH) - turns * TWO_PI_LOW
    s = r * r
    value = jnp.full_like(s, SINE[-1])
    for coefficient in SINE[-2::-1]:
        value = value * s + coefficient
    return value * r


def eliminate(block):
    rows = [block[8 * t : 8 * t + 8, :] for t in range(8)]
    below = lax.broadcasted_iota(jnp.int32, (8, 128), 0)
    for p in range(8):
        columns = {
            (t, k): jnp.broadcast_to(rows[t][:, 8 * p + k : 8 * p + k + 1], (8, 128))
            for t in range(p, 8)
            for k in range(8)
        }
        for k in range(8):
            inverse = 1.0 / jnp.broadcast_to(columns[p, k][k : k + 1, :], (8, 128))
            pivot_row = jnp.broadcast_to(rows[p][k : k + 1, :], (8, 128))
            entries = [
                jnp.broadcast_to(columns[p, later][k : k + 1, :], (8, 128))
                for later in range(k + 1, 8)
            ]
            for t in range(p, 8):
                factor = columns[t, k] * inverse
                if t == p:
                    factor = jnp.where(below > k, factor, 0.0)
                rows[t] = rows[t] - factor * pivot_row
                for later in range(k + 1, 8):
                    columns[t, later] = columns[t, later] - factor * entries[later - k - 1]
    return jnp.concatenate(rows, axis=0)


def factor_inverse(gram_ref, inverse_ref, work_ref):
    size = gram_ref.shape[0]
    work_ref[...] = gram_ref[...]
    row = lax.broadcasted_iota(jnp.int32, (size, size), 0)
    column = lax.broadcasted_iota(jnp.int32, (size, size), 1)
    inverse_ref[...] = jnp.where(row == column, 1.0, 0.0).astype(jnp.float32)
    lane = lax.broadcasted_iota(jnp.int32, (BLOCK, 128), 1)
    line = lax.broadcasted_iota(jnp.int32, (BLOCK, 128), 0)
    for start in range(0, size, BLOCK):
        own = slice(start, start + BLOCK)
        tile_start = start // 128 * 128
        tile = work_ref[own, tile_start : tile_start + 128]
        if start % 128:
            tile = pltpu.roll(tile, 64, 1)
        unit = jnp.where(lane - BLOCK == line, 1.0, 0.0)
        done = eliminate(jnp.where(lane < BLOCK, tile, unit))
        pivots = jnp.sum(jnp.where(lane == line, done, 0.0), axis=1, keepdims=True)
        scaled = pltpu.roll(done * lax.rsqrt(pivots), 64, 1)[:, :BLOCK]
        left = jnp.dot(scaled, work_ref[own, :], precision=HIGHEST, preferred_element_type=jnp.float32)
        right = jnp.dot(scaled, inverse_ref[own, :], precision=HIGHEST, preferred_element_type=jnp.float32)
        inverse_ref[own, :] = right
        rest = size - start - BLOCK
        if rest:
            lower = slice(start + BLOCK, size)
            flipped = left.T[start + BLOCK :, :]
            work_ref[lower, :] -= jnp.dot(flipped, left, precision=HIGHEST, preferred_element_type=jnp.float32)
            inverse_ref[lower, :] -= jnp.dot(flipped, right, precision=HIGHEST, preferred_element_type=jnp.float32)


MESH_ID = pl.DeviceIdType.MESH


def greet(peers):
    barrier = pltpu.get_barrier_semaphore()
    for peer in peers:
        pl.semaphore_signal(barrier, inc=1, device_id=peer, device_id_type=MESH_ID)
    pl.semaphore_wait(barrier, len(peers))


def sketch_and_gram(
    n_texel, n_light, tex_ref, feat_ref, sketch_ref, used_ref, count_ref, whole_ref, inverse_ref, tile_ref,
    logits, partial_ref,
    landed, whole, pieces, plane, column, gram, scaled, work,
    part_send, part_recv, plane_send, plane_recv, column_send, column_recv,
    full_send, full_recv, row_send, row_recv,
):
    texel, light = lax.axis_index("texel"), lax.axis_index("light")
    depth = partial_ref.shape[0] // n_light
    size = partial_ref.shape[1]
    piece = size // n_texel
    lights = [lax.rem(light + d, n_light) for d in range(n_light)]
    texels = [lax.rem(texel + d, n_texel) for d in range(n_texel)]
    greet([(texel, lights[d]) for d in range(1, n_light)] + [(texels[d], light) for d in range(1, n_texel)])

    def send(source, target, send_sem, recv_sem, device):
        copy = pltpu.make_async_remote_copy(
            src_ref=source, dst_ref=target, send_sem=send_sem, recv_sem=recv_sem,
            device_id=device, device_id_type=MESH_ID,
        )
        copy.start()
        return copy

    def rows_of(index, height):
        return pl.ds(pl.multiple_of(index * height, height), height)

    step = logits.shape[1]

    def fill(index):
        texels_here = tex_ref[rows_of(index, depth), :]

        def block(c, carry):
            columns = rows_of(c, step)
            logits[...] = lax.dot_general(
                texels_here, feat_ref[columns, :], (((1,), (1,)), ((), ())), preferred_element_type=jnp.float32
            )

            def strip(i, inner):
                value = bounded_sine(logits[rows_of(i, 16), :]).astype(jnp.bfloat16)
                tile_ref[pl.ds(pl.multiple_of(index * depth + i * 16, 16), 16), columns] = value
                return inner

            return lax.fori_loop(0, depth // 16, strip, carry, unroll=2)

        lax.fori_loop(0, feat_ref.shape[0] // step, block, 0)
        rows = rows_of(index, depth)
        partial_ref[rows, :] = (
            jnp.dot(tile_ref[rows, :], sketch_ref[...], preferred_element_type=jnp.float32) * used_ref[rows, :]
        )

    copies = []
    for d in range(1, n_light):
        fill(lights[d])
        copies.append(
            send(
                partial_ref.at[rows_of(lights[d], depth)], landed.at[d],
                part_send.at[d], part_recv.at[d], (texel, lights[d]),
            )
        )
    fill(light)
    own = partial_ref[rows_of(light, depth), :]
    for d, copy in enumerate(copies, 1):
        copy.wait()
        own = own + landed[d]
    whole[rows_of(light, depth), :] = own
    early = depth // 4

    def gather(part, first, height):
        rows = pl.ds(pl.multiple_of(light * depth + first, 8), height)
        return [
            send(
                whole.at[rows], whole.at[rows], full_send.at[part, d], full_recv.at[part, d], (texel, lights[d])
            )
            for d in range(1, n_light)
        ]

    gathers = gather(0, 0, early)
    local = lax.dot_general(
        own, own, (((0,), (0,)), ((), ())), precision=HIGHEST, preferred_element_type=jnp.float32
    )
    for index in range(n_texel):
        pieces[index] = local[index * piece : (index + 1) * piece, :]
    copies = [
        send(pieces.at[texels[d]], plane.at[d], plane_send.at[d], plane_recv.at[d], (texels[d], light))
        for d in range(1, n_texel)
    ]
    total = pieces[texel]
    for d, copy in enumerate(copies, 1):
        copy.wait()
        total = total + plane[d]
    column[light] = total
    copies = [
        send(column.at[light], column.at[light], column_send.at[d], column_recv.at[d], (texel, lights[d]))
        for d in range(1, n_light)
    ]
    for copy in copies:
        copy.wait()
    gathers += gather(1, early, depth - early)
    total = column[0]
    for index in range(1, n_light):
        total = total + column[index]
    gram[rows_of(texel, piece), :] = total
    copies = [
        send(
            gram.at[rows_of(texel, piece)], gram.at[rows_of(texel, piece)],
            row_send.at[d], row_recv.at[d], (texels[d], light),
        )
        for d in range(1, n_texel)
    ]
    for copy in copies:
        copy.wait()
    scaled[...] = gram[...] / count_ref[...]
    factor_inverse(scaled, inverse_ref, work)
    for copy in gathers:
        copy.wait()
    whole_ref[...] = whole[...]


def reduced(tex_feat, light_feat, sketch, used, count, n_texel, n_light):
    capacity, size = tex_feat.shape[0], sketch.shape[1]
    lights = light_feat.shape[0]
    step = next(w for w in (512, 256, 128) if lights % w == 0)
    depth, piece = capacity // n_light, size // n_texel
    vmem = pl.BlockSpec(memory_space=pltpu.VMEM)
    f32 = jnp.float32
    sems = pltpu.SemaphoreType.DMA
    return pl.pallas_call(
        functools.partial(sketch_and_gram, n_texel, n_light),
        out_shape=(
            jax.ShapeDtypeStruct((capacity, size), f32),
            jax.ShapeDtypeStruct((size, size), f32),
            jax.ShapeDtypeStruct((capacity, lights), jnp.bfloat16),
        ),
        in_specs=[vmem] * 5,
        out_specs=(vmem, vmem, vmem),
        scratch_shapes=[
            pltpu.VMEM((depth, step), f32),
            pltpu.VMEM((capacity, size), f32),
            pltpu.VMEM((n_light, depth, size), f32),
            pltpu.VMEM((capacity, size), f32),
            pltpu.VMEM((n_texel, piece, size), f32),
            pltpu.VMEM((n_texel, piece, size), f32),
            pltpu.VMEM((n_light, piece, size), f32),
            pltpu.VMEM((size, size), f32),
            pltpu.VMEM((size, size), f32),
            pltpu.VMEM((size, size), f32),
            sems((n_light,)), sems((n_light,)),
            sems((n_texel,)), sems((n_texel,)),
            sems((n_light,)), sems((n_light,)),
            sems((2, n_light)), sems((2, n_light)),
            sems((n_texel,)), sems((n_texel,)),
        ],
        compiler_params=pltpu.CompilerParams(collective_id=1, has_side_effects=True),
    )(tex_feat, light_feat, sketch, used, count)


def halving_order(bits, last_first):
    rest = list(range(1, bits))
    return [0] + (rest[::-1] if last_first else rest)


def scatter_sum(n_texel, partial_ref, out_ref, held, landed, send_sem, recv_sem):
    texel, light = lax.axis_index("texel"), lax.axis_index("light")
    bits = n_texel.bit_length() - 1
    bit = [lax.rem(texel // (1 << b), 2) for b in range(bits)]
    partner = [texel + (1 - 2 * bit[b]) * (1 << b) for b in range(bits)]
    greet([(partner[b], light) for b in range(bits)])
    piece = partial_ref.shape[0] // n_texel
    width = partial_ref.shape[1] // 2

    def start_of(mask):
        block = 0
        for b in range(bits):
            flipped = 1 - bit[b] if mask >> b & 1 else bit[b]
            block = block + flipped * (1 << b)
        return pl.multiple_of(block * piece, piece)

    orders = [halving_order(bits, False), halving_order(bits, True)]
    flights = [{}, {}]
    for step in range(bits):
        for half, order in enumerate(orders):
            b = order[step]
            left = [m for m in range(n_texel) if all(not m >> done & 1 for done in order[:step])]
            later = order[step + 1 :]
            going = [m for m in left if m >> b & 1]
            going.sort(key=lambda m: [-(m >> c & 1) for c in later])
            columns = pl.ds(half * width, width)
            for m in going:
                kept = m - (1 << b)
                if step == 0:
                    source = partial_ref.at[pl.ds(start_of(m), piece), columns]
                else:
                    arrived = flights[half].pop((step - 1, m))
                    arrived.wait()
                    below = (
                        partial_ref[pl.ds(start_of(m), piece), columns] if step == 1 else held[half, m]
                    )
                    held[half, m] = below + landed[half, step - 1, m]
                    source = held.at[half, m]
                copy = pltpu.make_async_remote_copy(
                    src_ref=source,
                    dst_ref=landed.at[half, step, kept],
                    send_sem=send_sem.at[half, step, kept],
                    recv_sem=recv_sem.at[half, step, kept],
                    device_id=(partner[b], light),
                    device_id_type=MESH_ID,
                )
                copy.start()
                flights[half][step, kept] = copy
        if step:
            for half, order in enumerate(orders):
                for key in [k for k in flights[half] if k[0] == step - 1]:
                    m = key[1]
                    flights[half].pop(key).wait()
                    columns = pl.ds(half * width, width)
                    below = (
                        partial_ref[pl.ds(start_of(m), piece), columns] if step == 1 else held[half, m]
                    )
                    held[half, m] = below + landed[half, step - 1, m]
    for half in range(2):
        columns = pl.ds(half * width, width)
        flights[half].pop((bits - 1, 0)).wait()
        below = partial_ref[pl.ds(start_of(0), piece), columns] if bits == 1 else held[half, 0]
        out_ref[:, half * width : (half + 1) * width] = below + landed[half, bits - 1, 0]


def scattered(partial, n_texel):
    size, lights = partial.shape
    piece, width, bits = size // n_texel, lights // 2, n_texel.bit_length() - 1
    vmem = pl.BlockSpec(memory_space=pltpu.VMEM)
    return pl.pallas_call(
        functools.partial(scatter_sum, n_texel),
        out_shape=jax.ShapeDtypeStruct((piece, lights), jnp.float32),
        in_specs=[vmem],
        out_specs=vmem,
        scratch_shapes=[
            pltpu.VMEM((2, n_texel, piece, width), jnp.float32),
            pltpu.VMEM((2, bits, n_texel, piece, width), jnp.float32),
            pltpu.SemaphoreType.DMA((2, bits, n_texel)),
            pltpu.SemaphoreType.DMA((2, bits, n_texel)),
        ],
        compiler_params=pltpu.CompilerParams(collective_id=2, has_side_effects=True),
    )(partial)


def on_device(n_texel, n_light, tex_feat, light_feat, sketch, row_counts):
    capacity = tex_feat.shape[0]
    own_count = row_counts[lax.axis_index("texel")]
    valid_total = jnp.sum(row_counts).astype(jnp.float32)
    row_valid = (lax.iota(jnp.int32, capacity) < own_count).astype(jnp.float32)
    count = jnp.full((1, sketch.shape[1]), valid_total)
    sketched, inverse, tile_block = reduced(
        tex_feat, light_feat, sketch, row_valid[:, None], count, n_texel, n_light
    )
    basis = lax.dot_general(sketched, inverse, (((1,), (1,)), ((), ())), precision=HIGHEST)
    basis_half = basis.astype(jnp.bfloat16)
    partial_coeffs = lax.dot_general(
        basis_half, tile_block, (((0,), (0,)), ((), ())), preferred_element_type=jnp.float32
    )
    coeffs = scattered(partial_coeffs, n_texel) / jnp.sqrt(valid_total)
    return (basis, coeffs)


def solution(mesh):
    placed = (P("texel", None), P("light", None), P("light", None), P())
    return jax.shard_map(
        functools.partial(on_device, mesh.shape["texel"], mesh.shape["light"]),
        mesh=mesh,
        in_specs=placed,
        out_specs=(P("texel", None), P("texel", "light")),
        check_vma=False,
    )
```
